32 devices in a mesh: grp: 8 (over z, y), rep: 4 (over x, core).
Axes of the slice: x: 2, y: 2, z: 4, core: 2. Of those that a mesh axis runs over, the one named last changes fastest.
Arguments:
- queries: bfloat16 [16, 4, 32, 128], P('grp', 'rep'), may hold values from -3.2 to 3.2
- passages: bfloat16 [512, 4, 180, 128], P('grp', 'rep'), may hold values from -1.796875 to 1.796875
- lengths: int32 [512, 4], P('grp', 'rep'), may hold values from 16 to 180
- cand_ids: int32 [16, 4, 64], P('grp', 'rep'), may hold values from 0 to 511, as said below
- owner_map: int32 [4, 512], P('rep'), may hold values from 0 to 511, as said below
- teacher: float32 [16, 4, 64], P('grp', 'rep'), may hold values from -12 to 312
- weights: float32 [16, 4], P('grp', 'rep'), may hold values from 0.5 to 18
Outputs:
- loss: float32 [], replicated
- query_grad: float32 [16, 4, 32, 128], P('grp', 'rep')
- passage_grad: bfloat16 [512, 4, 180, 128], P('grp', 'rep')
The draws below stay inside these ranges and needn't reach their ends.
Inputs may be any that keep to these rules, and one draw needn't show every extreme that they name: `cand_ids`: within each replica, the 128 candidates of the queries of one grp index have storage rows of which at most 32 (counted with repeats) lie in any one aligned block of 64 rows; in every draw, in each replica, one block receives exactly 32 from every grp index. `owner_map`: each row is a permutation of 0 to 511.
All inputs are finite; a program needn't handle non-finite values.
Results may differ from the reference program's by a relative error of at most 0.0055.
Values may be sent and summed in bfloat16 or wider, within the bound.
A program may use at most 128 MiB of HBM per device.

```python
import math
import jax
import jax.numpy as jnp
from jax import lax

DIM = 128
QL = 32
PL = 180
NWAY = 64
Q_DEV = 2
P_DEV = 64
GROUPS = 8
REPS = 4
QUERIES = 16
PASSAGES = 512


def routing(key):
    ref_count = Q_DEV * NWAY
    capacity = 2 * ref_count // GROUPS
    pool_size = GROUPS * capacity
    keys = jax.random.split(jax.random.fold_in(key, 7), 5)
    hot_owner = jax.random.randint(keys[0], (REPS,), 0, GROUPS)
    pool_owner = jnp.arange(pool_size, dtype=jnp.int32) // capacity
    priority = jax.random.randint(keys[1], (GROUPS, REPS, pool_size), 0, 1 << 20) * pool_size + jnp.arange(pool_size, dtype=jnp.int32)
    is_hot = pool_owner[None, None, :] == hot_owner[None, :, None]
    priority = jnp.where(is_hot, jnp.arange(pool_size, dtype=jnp.int32) - pool_size, priority)
    order = jnp.argsort(priority, axis=-1)[..., :ref_count]
    owners = pool_owner[order]
    shuffle_key = jax.random.randint(keys[2], (GROUPS, REPS, ref_count), 0, 1 << 20) * ref_count + jnp.arange(ref_count, dtype=jnp.int32)
    shuffle = jnp.argsort(shuffle_key, axis=-1)
    owners = jnp.take_along_axis(owners, shuffle, axis=-1)
    slot_rows = jax.random.randint(keys[3], (GROUPS, REPS, ref_count), 0, P_DEV)
    storage = owners * P_DEV + slot_rows
    perm_keys = jax.random.split(keys[4], REPS)
    owner_table = jax.vmap(lambda one_key: jax.random.permutation(one_key, P_DEV * GROUPS))(perm_keys).astype(jnp.int32)
    inverse = jnp.argsort(owner_table, axis=-1).astype(jnp.int32)
    wide_inverse = jnp.broadcast_to(inverse[None], (GROUPS, REPS, P_DEV * GROUPS))
    identity = jnp.take_along_axis(wide_inverse, storage, axis=-1)
    candidate_ids = identity.reshape(GROUPS, REPS, Q_DEV, NWAY).transpose(0, 2, 1, 3).reshape(GROUPS * Q_DEV, REPS, NWAY)
    return (candidate_ids.astype(jnp.int32), owner_table)


def draw_cand_ids(key, part):
    return routing(key)[0]


def draw_owner_map(key, part):
    return routing(key)[1]


def draw_queries(key, part):
    keys = jax.random.split(jax.random.fold_in(key, 11), 2)
    shape = (QUERIES, REPS, QL, DIM)
    normal_part = jnp.clip(jax.random.normal(keys[0], shape, jnp.float32), -3.5, 3.5)
    row_scale = jnp.exp(jax.random.uniform(keys[1], (QUERIES, REPS, 1, 1), jnp.float32, math.log(0.03), math.log(3.0)))
    return (0.3 * normal_part * row_scale).astype(jnp.bfloat16)


def draw_teacher(key, part):
    keys = jax.random.split(jax.random.fold_in(key, 13), 1)
    normal_part = 2.0 * jnp.clip(jax.random.normal(keys[0], (QUERIES, REPS, NWAY), jnp.float32), -6.0, 6.0)
    return normal_part


def draw_weights(key, part):
    keys = jax.random.split(jax.random.fold_in(key, 17), 1)
    query_index = jnp.arange(QUERIES, dtype=jnp.int32)[:, None]
    replica_index = jnp.arange(REPS, dtype=jnp.int32)[None, :]
    device_index = query_index // Q_DEV * REPS + replica_index
    ramp = 1.0 + 2.0 * device_index.astype(jnp.float32) / (GROUPS * REPS - 1)
    return jnp.exp(jax.random.uniform(keys[0], (QUERIES, REPS), jnp.float32, math.log(0.5), math.log(2.0))) * ramp


def place_ends(values, stream_key, low, largest):
    longest = values.shape.index(max(values.shape))
    spots = []
    for shift in (0, 1):
        where = [jax.random.randint(jax.random.fold_in(stream_key, axis), (), 0, length) for axis, length in enumerate(values.shape)]
        where[longest] = (where[longest] + shift) % values.shape[longest]
        spots.append(tuple(where))
    return values.at[spots[0]].set(low).at[spots[1]].set(largest)


def block_levels(key, shape, pieces, low, top_value):
    loudness = 1.0
    for position, shards_of in pieces:
        heights = jax.random.uniform(jax.random.fold_in(jax.random.fold_in(key, 6), position), (shards_of,), jnp.float32, low / len(pieces), top_value / len(pieces))
        loudness = loudness * jnp.repeat(jnp.exp(heights), shape[position] // shards_of).reshape((-1,) + (1,) * (len(shape) - 1 - position))
    return loudness


def gaussian(rng, extent, width, bound, shards=(), held_as=jnp.bfloat16):
    entries = width * jax.random.normal(rng, extent, jnp.float32)
    if shards:
        entries = entries * block_levels(rng, extent, shards, -0.22, 0.18)
    return jnp.clip(entries, -bound, bound).astype(held_as)


def setup_inputs(seed: int = 0) -> dict:
    seeds = jax.random.split(jax.random.key(seed), 8)
    return {
        "queries": draw_queries(jax.random.fold_in(seeds[7], 71), 0),
        "passages": gaussian(seeds[1], (PASSAGES, REPS, PL, DIM), 0.3, 1.796875, ((0, 8), (1, 4))),
        "lengths": place_ends(jax.random.randint(seeds[2], (PASSAGES, REPS), 16, PL + 1), jax.random.fold_in(seeds[2], 1), 16, PL).astype(jnp.int32),
        "cand_ids": draw_cand_ids(jax.random.fold_in(seeds[7], 71), 0),
        "owner_map": draw_owner_map(jax.random.fold_in(seeds[7], 71), 0),
        "teacher": draw_teacher(jax.random.fold_in(seeds[7], 71), 0),
        "weights": draw_weights(jax.random.fold_in(seeds[7], 71), 0),
    }


temper = 0.05


def rounded(values):
    return lax.optimization_barrier(values.astype(jnp.bfloat16)).astype(jnp.float32)


def token_softmax(products, lengths_used):
    usable = lax.broadcasted_iota(jnp.int32, products.shape, products.ndim - 1) < lengths_used[..., None, None]
    scaled = jnp.where(usable, products / temper, -1e30)
    highest = jnp.max(scaled, axis=-1, keepdims=True)
    powers = jnp.where(usable, jnp.exp(scaled - highest), 0.0)
    summed = jnp.sum(powers, axis=-1, keepdims=True)
    matched = temper * (highest[..., 0] + jnp.log(summed[..., 0]))
    return matched, powers / summed


def pair_terms(query_tokens, passage_tokens, lengths_used):
    products = jnp.einsum("id,cjd->cij", query_tokens.astype(jnp.float32), passage_tokens.astype(jnp.float32))
    matched, attention = token_softmax(products, lengths_used)
    return jnp.sum(matched, axis=-1), attention


def reference(queries, passages, lengths, cand_ids, owner_map, teacher, weights):
    query_count = queries.shape[0]
    replicas = queries.shape[1]

    def fetch_blocks(query_row, replica):
        storage_rows = owner_map[replica][cand_ids[query_row, replica]]
        return storage_rows, passages[storage_rows, replica], lengths[storage_rows, replica]

    def score_one(flat_index):
        query_row = flat_index // replicas
        replica = flat_index % replicas
        storage_rows, blocks, lengths_used = fetch_blocks(query_row, replica)
        return pair_terms(queries[query_row, replica], blocks, lengths_used)[0]

    student = lax.map(score_one, jnp.arange(query_count * replicas, dtype=jnp.int32))
    student = student.reshape(query_count, replicas, -1)
    log_student = jax.nn.log_softmax(student, axis=-1)
    log_teacher = jax.nn.log_softmax(teacher, axis=-1)
    teacher_prob = jnp.exp(log_teacher)
    divergence = jnp.sum(teacher_prob * (log_teacher - log_student), axis=-1)
    weight_sum = jnp.sum(weights)
    loss_value = jnp.sum(weights * divergence) / weight_sum
    score_grad = (query_count * replicas) * weights[..., None] / weight_sum * (jnp.exp(log_student) - teacher_prob)
    query_parts = []
    passage_parts = []
    for replica in range(replicas):
        def backward(accum_grad, query_row):
            storage_rows, blocks, lengths_used = fetch_blocks(query_row, replica)
            query_tokens = queries[query_row, replica]
            unused, attention = pair_terms(query_tokens, blocks, lengths_used)
            scaled_grad = rounded(score_grad[query_row, replica][:, None, None] * attention)
            pair_query = rounded(jnp.einsum("cij,cjd->cid", scaled_grad, blocks.astype(jnp.float32)))
            query_part = jnp.sum(pair_query, axis=0)
            pair_passage = rounded(jnp.einsum("cij,id->cjd", scaled_grad, query_tokens.astype(jnp.float32)))
            accum_grad = accum_grad.at[storage_rows].add(pair_passage)
            return accum_grad, query_part

        initial = jnp.zeros((passages.shape[0],) + passages.shape[2:], jnp.float32)
        summed, replica_grads = lax.scan(backward, initial, jnp.arange(query_count, dtype=jnp.int32))
        query_parts.append(replica_grads)
        passage_parts.append(summed.astype(jnp.bfloat16))
    return loss_value, jnp.stack(query_parts, axis=1), jnp.stack(passage_parts, axis=1)
```

```python
import functools
import math

import jax
import jax.numpy as jnp
from jax import lax
from jax.experimental import pallas as pl
from jax.experimental.pallas import tpu as pltpu
from jax.sharding import PartitionSpec as P

temper = 0.05
to_base2 = 1.0 / (temper * math.log(2.0))
LANES = 128
MESH = pl.DeviceIdType.MESH
HIGH = lax.Precision.HIGHEST
VMEM_SPEC = pl.BlockSpec(memory_space=pltpu.VMEM)


def greet(groups, replicas, me, mine):
    barrier = pltpu.get_barrier_semaphore()
    for step in range(1, groups):
        pl.semaphore_signal(
            barrier, inc=1, device_id={"grp": lax.rem(me + step, groups)}, device_id_type=MESH
        )
    for step in range(1, replicas):
        pl.semaphore_signal(
            barrier, inc=1, device_id={"rep": lax.rem(mine + step, replicas)}, device_id_type=MESH
        )
    pl.semaphore_wait(barrier, groups - 1 + replicas - 1)


def share_kernel(
    groups, block, queries_ref, cand_ref, map_ref, teacher_ref, weights_ref,
    all_queries, all_meta, query_buf, meta_buf, send_sem, recv_sem,
):
    me = lax.axis_index("grp")
    count, ways = cand_ref.shape
    table = map_ref[...].astype(jnp.float32)
    ids = lax.broadcasted_iota(jnp.int32, (ways, table.shape[1]), 1)
    diagonal = lax.broadcasted_iota(jnp.int32, (ways, ways), 0) == lax.broadcasted_iota(
        jnp.int32, (ways, ways), 1
    )
    teacher = teacher_ref[...]
    top = jnp.max(teacher, axis=1, keepdims=True)
    log_teacher = teacher - top
    log_teacher = log_teacher - jnp.log(jnp.sum(jnp.exp(log_teacher), axis=1, keepdims=True))
    prob = jnp.exp(log_teacher)
    entropy = jnp.sum(prob * log_teacher, axis=1, keepdims=True)
    meta_buf[me] = jnp.zeros(meta_buf.shape[1:], jnp.float32)
    for q in range(count):
        line = cand_ref[q : q + 1, :].astype(jnp.float32)
        column = jnp.sum(jnp.where(diagonal, line, 0.0), axis=1, keepdims=True).astype(jnp.int32)
        row = jnp.sum(jnp.where(column == ids, table, 0.0), axis=1, keepdims=True)
        row = jnp.sum(jnp.where(diagonal, row, 0.0), axis=0, keepdims=True)
        meta_buf[me, q : q + 1, :ways] = row
    meta_buf[me, count : 2 * count, :ways] = prob
    meta_buf[me, 2 * count : 3 * count, :] = jnp.broadcast_to(weights_ref[...], (count, LANES))
    meta_buf[me, 3 * count : 4 * count, :] = jnp.broadcast_to(entropy, (count, LANES))
    query_buf[me] = queries_ref[...]
    greet(groups, 1, me, 0)
    copies = []
    for step in range(1, groups):
        peer = lax.rem(me + step, groups)
        for which, buf in enumerate((query_buf, meta_buf)):
            copies.append(
                pltpu.make_async_remote_copy(
                    src_ref=buf.at[me],
                    dst_ref=buf.at[me],
                    send_sem=send_sem.at[which, step],
                    recv_sem=recv_sem.at[which, step],
                    device_id={"grp": peer},
                    device_id_type=MESH,
                )
            )
            copies[-1].start()
    for copy in copies:
        copy.wait()
    all_queries[...] = query_buf[...]
    all_meta[...] = meta_buf[...]


def forward_kernel(
    per_step, count, ways, block, lengths_ref, passages_ref, queries_ref, meta_ref,
    lse_ref, score_ref, hits_ref, mass_ref,
):
    step = pl.program_id(0)
    groups = meta_ref.shape[0]
    tokens = passages_ref.shape[1]
    slot = score_ref.shape[1]

    @pl.when(step == 0)
    def _():
        spots = lax.broadcasted_iota(jnp.int32, (ways, groups * slot), 1)
        for source in range(groups):
            turned = jnp.transpose(meta_ref[source])
            for q in range(count):
                row = turned[:ways, q : q + 1].astype(jnp.int32)
                spot = row + (slot - block) * (row // block)
                hot = spot == spots
                place = source * count + q
                hits_ref[place : place + 1, :] = jnp.sum(
                    jnp.where(hot, 1.0, 0.0), axis=0, keepdims=True
                )
                mass_ref[place : place + 1, :] = jnp.sum(
                    jnp.where(hot, turned[:ways, count + q : count + q + 1], 0.0),
                    axis=0,
                    keepdims=True,
                )

    position = lax.broadcasted_iota(jnp.int32, (tokens, 1), 0)
    for k in range(per_step):
        length = lengths_ref[step * per_step + k]
        products = lax.dot_general(
            passages_ref[k], queries_ref[...], (((1,), (1,)), ((), ())),
            preferred_element_type=jnp.float32,
        )
        scaled = jnp.where(position < length, products * to_base2, -1e30)
        highest = jnp.max(scaled, axis=0, keepdims=True)
        summed = jnp.sum(jnp.exp2(scaled - highest), axis=0, keepdims=True)
        lse_ref[step * per_step + k, :, :] = highest + jnp.log2(summed)

    @pl.when(step == pl.num_programs(0) - 1)
    def _():
        total, width = score_ref.shape[0], lse_ref.shape[2]
        each = width // total
        belongs = lax.broadcasted_iota(jnp.int32, (total, width), 1) // each
        pick = jnp.where(
            belongs == lax.broadcasted_iota(jnp.int32, (total, width), 0), 1.0, 0.0
        )
        matched = lse_ref[:, 0, :] * (1.0 / to_base2)
        score_ref[...] = jnp.zeros_like(score_ref)
        score_ref[:, : lse_ref.shape[0]] = lax.dot_general(
            pick, matched, (((1,), (1,)), ((), ())),
            precision=HIGH, preferred_element_type=jnp.float32,
        )


def grade_kernel(
    groups, replicas, score_ref, hits_ref, mass_ref, meta_ref, grad_ref, loss_ref,
    score_buf, weight_buf, grad_buf, query_weight, query_entropy,
    send_sem, recv_sem, wsend_sem, wrecv_sem,
):
    me = lax.axis_index("grp")
    mine = lax.axis_index("rep")
    total, slot = score_ref.shape
    count = total // groups
    for source in range(groups):
        span = slice(source * count, (source + 1) * count)
        query_weight[span, :] = meta_ref[source, 2 * count : 3 * count, :]
        query_entropy[span, :] = meta_ref[source, 3 * count : 4 * count, :]
    weights = query_weight[:, :1]
    score_buf[me] = score_ref[...]
    weight_buf[mine] = jnp.broadcast_to(
        jnp.sum(query_weight[...], axis=0, keepdims=True), weight_buf.shape[1:]
    )
    greet(groups, replicas, me, mine)
    copies = []
    for step in range(1, groups):
        copies.append(
            pltpu.make_async_remote_copy(
                src_ref=score_buf.at[me],
                dst_ref=score_buf.at[me],
                send_sem=send_sem.at[step],
                recv_sem=recv_sem.at[step],
                device_id={"grp": lax.rem(me + step, groups)},
                device_id_type=MESH,
            )
        )
        copies[-1].start()
    for step in range(1, replicas):
        copies.append(
            pltpu.make_async_remote_copy(
                src_ref=weight_buf.at[mine],
                dst_ref=weight_buf.at[mine],
                send_sem=wsend_sem.at[step],
                recv_sem=wrecv_sem.at[step],
                device_id={"rep": lax.rem(mine + step, replicas)},
                device_id_type=MESH,
            )
        )
        copies[-1].start()
    for copy in copies:
        copy.wait()
    weight_sum = jnp.sum(weight_buf[...], axis=0)[:1, :1]
    scores = jnp.concatenate([score_buf[owner] for owner in range(groups)], axis=1)
    hits = hits_ref[...]
    mass = mass_ref[...]
    asked = hits > 0.0
    held = jnp.where(asked, scores, -1e30)
    highest = jnp.max(held, axis=1, keepdims=True)
    summed = jnp.sum(hits * jnp.exp(held - highest), axis=1, keepdims=True)
    log_student = jnp.where(asked, scores - (highest + jnp.log(summed)), -1e30)
    student = hits * jnp.exp(log_student)
    crossed = jnp.sum(jnp.where(asked, mass * log_student, 0.0), axis=1, keepdims=True)
    divergence = query_entropy[:, :1] - crossed
    grad_buf[...] = (total * replicas) * weights / weight_sum * (student - mass)
    own = grad_buf[:, pl.ds(pl.multiple_of(me * slot, slot), slot)]
    width = grad_ref.shape[2]
    each = width // total
    belongs = lax.broadcasted_iota(jnp.int32, (total, width), 1) // each
    pick = jnp.where(belongs == lax.broadcasted_iota(jnp.int32, (total, width), 0), 1.0, 0.0)
    spread = lax.dot_general(
        own, pick, (((0,), (0,)), ((), ())), precision=HIGH, preferred_element_type=jnp.float32
    )
    grad_ref[:, 0, :] = spread[: grad_ref.shape[0]]
    loss_ref[...] = jnp.broadcast_to(
        jnp.sum(weights * divergence, axis=0, keepdims=True) / weight_sum, loss_ref.shape
    )


def backward_kernel(
    per_step, lengths_ref, passages_ref, queries_ref, lse_ref, grad_ref, out_ref, partial_ref, total
):
    step = pl.program_id(0)
    tokens = passages_ref.shape[1]

    @pl.when(step == 0)
    def _():
        total[...] = jnp.zeros_like(total)

    position = lax.broadcasted_iota(jnp.int32, (tokens, 1), 0)
    queries = queries_ref[...]
    added = None
    for k in range(per_step):
        usable = position < lengths_ref[step * per_step + k]
        passage = passages_ref[k]
        products = lax.dot_general(
            passage, queries, (((1,), (1,)), ((), ())), preferred_element_type=jnp.float32
        )
        powers = jnp.exp2(jnp.minimum(products * to_base2 - lse_ref[k], 0.0))
        scaled_grad = (powers * grad_ref[k]).astype(jnp.bfloat16)
        token_grad = jnp.dot(scaled_grad, queries, preferred_element_type=jnp.float32)
        out_ref[k] = jnp.where(usable, token_grad, 0.0).astype(jnp.bfloat16)
        kept = jnp.where(usable, passage.astype(jnp.float32), 0.0).astype(jnp.bfloat16)
        part = lax.dot_general(
            scaled_grad, kept, (((0,), (0,)), ((), ())), preferred_element_type=jnp.float32
        )
        added = part if added is None else added + part
    total[...] += added

    @pl.when(step == pl.num_programs(0) - 1)
    def _():
        partial_ref[...] = total[...].astype(partial_ref.dtype)


def collect_kernel(
    groups, replicas, partial_ref, loss_ref, grad_ref, loss_out,
    arrived, loss_buf, send_sem, recv_sem, lsend_sem, lrecv_sem,
):
    me = lax.axis_index("grp")
    mine = lax.axis_index("rep")
    loss_buf[mine] = loss_ref[...]
    greet(groups, replicas, me, mine)
    copies = []
    for step in range(1, groups):
        peer = lax.rem(me + step, groups)
        copies.append(
            pltpu.make_async_remote_copy(
                src_ref=partial_ref.at[peer],
                dst_ref=arrived.at[me],
                send_sem=send_sem.at[step],
                recv_sem=recv_sem.at[step],
                device_id={"grp": peer},
                device_id_type=MESH,
            )
        )
        copies[-1].start()
    for step in range(1, replicas):
        copies.append(
            pltpu.make_async_remote_copy(
                src_ref=loss_buf.at[mine],
                dst_ref=loss_buf.at[mine],
                send_sem=lsend_sem.at[step],
                recv_sem=lrecv_sem.at[step],
                device_id={"rep": lax.rem(mine + step, replicas)},
                device_id_type=MESH,
            )
        )
        copies[-1].start()
    arrived[me] = partial_ref[me]
    for copy in copies:
        copy.wait()
    grad_ref[...] = jnp.sum(arrived[...].astype(jnp.float32), axis=0)
    loss_out[...] = jnp.sum(loss_buf[...], axis=0)


def on_device(queries, passages, lengths, cand_ids, owner_map, teacher, weights):
    groups = lax.axis_size("grp")
    replicas = lax.axis_size("rep")
    count, _, query_len, dim = queries.shape
    block, _, tokens, _ = passages.shape
    ways = cand_ids.shape[2]
    own_rows = count * query_len
    width = groups * own_rows
    total = groups * count
    slot = -(-block // LANES) * LANES
    f32 = jnp.float32
    dma = pltpu.SemaphoreType.DMA
    meta_rows = -(-4 * count // 8) * 8
    all_queries, all_meta = pl.pallas_call(
        functools.partial(share_kernel, groups, block),
        name="share",
        out_shape=[
            jax.ShapeDtypeStruct((groups, own_rows, dim), queries.dtype),
            jax.ShapeDtypeStruct((groups, meta_rows, LANES), f32),
        ],
        in_specs=[VMEM_SPEC] * 5,
        out_specs=[VMEM_SPEC] * 2,
        scratch_shapes=[
            pltpu.VMEM((groups, own_rows, dim), queries.dtype),
            pltpu.VMEM((groups, meta_rows, LANES), f32),
            dma((2, groups)),
            dma((2, groups)),
        ],
        compiler_params=pltpu.CompilerParams(collective_id=0, has_side_effects=True),
    )(
        queries.reshape(own_rows, dim),
        cand_ids[:, 0],
        owner_map,
        teacher[:, 0],
        weights,
    )
    flat_queries = all_queries.reshape(width, dim)
    flat_passages = passages.reshape(block, tokens, dim)
    flat_lengths = lengths.reshape(block)
    per_step = 4 if block % 4 == 0 else 1
    steps = block // per_step
    whole = lambda *shape: pl.BlockSpec(shape, lambda i, *_: (0,) * len(shape))
    passage_spec = pl.BlockSpec((per_step, tokens, dim), lambda i, *_: (i, 0, 0))
    row_spec = pl.BlockSpec((per_step, 1, width), lambda i, *_: (i, 0, 0))
    lse, score, hits, mass = pl.pallas_call(
        functools.partial(forward_kernel, per_step, count, ways, block),
        name="forward",
        grid_spec=pltpu.PrefetchScalarGridSpec(
            num_scalar_prefetch=1,
            grid=(steps,),
            in_specs=[passage_spec, whole(width, dim), whole(groups, meta_rows, LANES)],
            out_specs=[
                whole(block, 1, width),
                whole(total, slot),
                whole(total, groups * slot),
                whole(total, groups * slot),
            ],
        ),
        out_shape=[
            jax.ShapeDtypeStruct((block, 1, width), f32),
            jax.ShapeDtypeStruct((total, slot), f32),
            jax.ShapeDtypeStruct((total, groups * slot), f32),
            jax.ShapeDtypeStruct((total, groups * slot), f32),
        ],
        compiler_params=pltpu.CompilerParams(dimension_semantics=("arbitrary",)),
    )(flat_lengths, flat_passages, flat_queries, all_meta)
    grad, loss_part = pl.pallas_call(
        functools.partial(grade_kernel, groups, replicas),
        name="grade",
        out_shape=[
            jax.ShapeDtypeStruct((block, 1, width), f32),
            jax.ShapeDtypeStruct((8, LANES), f32),
        ],
        in_specs=[VMEM_SPEC] * 4,
        out_specs=[VMEM_SPEC] * 2,
        scratch_shapes=[
            pltpu.VMEM((groups, total, slot), f32),
            pltpu.VMEM((replicas, 8, LANES), f32),
            pltpu.VMEM((total, groups * slot), f32),
            pltpu.VMEM((total, LANES), f32),
            pltpu.VMEM((total, LANES), f32),
            dma((groups,)),
            dma((groups,)),
            dma((replicas,)),
            dma((replicas,)),
        ],
        compiler_params=pltpu.CompilerParams(collective_id=1, has_side_effects=True),
    )(score, hits, mass, all_meta)
    passage_grad, partial = pl.pallas_call(
        functools.partial(backward_kernel, per_step),
        name="backward",
        grid_spec=pltpu.PrefetchScalarGridSpec(
            num_scalar_prefetch=1,
            grid=(steps,),
            in_specs=[passage_spec, whole(width, dim), row_spec, row_spec],
            out_specs=[passage_spec, whole(width, dim)],
            scratch_shapes=[pltpu.VMEM((width, dim), f32)],
        ),
        out_shape=[
            jax.ShapeDtypeStruct((block, tokens, dim), jnp.bfloat16),
            jax.ShapeDtypeStruct((width, dim), jnp.bfloat16),
        ],
        compiler_params=pltpu.CompilerParams(dimension_semantics=("arbitrary",)),
    )(flat_lengths, flat_passages, flat_queries, lse, grad)
    query_grad, loss = pl.pallas_call(
        functools.partial(collect_kernel, groups, replicas),
        name="collect",
        out_shape=[
            jax.ShapeDtypeStruct((own_rows, dim), f32),
            jax.ShapeDtypeStruct((8, LANES), f32),
        ],
        in_specs=[VMEM_SPEC] * 2,
        out_specs=[VMEM_SPEC] * 2,
        scratch_shapes=[
            pltpu.VMEM((groups, own_rows, dim), jnp.bfloat16),
            pltpu.VMEM((replicas, 8, LANES), f32),
            dma((groups,)),
            dma((groups,)),
            dma((replicas,)),
            dma((replicas,)),
        ],
        compiler_params=pltpu.CompilerParams(collective_id=2, has_side_effects=True),
    )(partial.reshape(groups, own_rows, dim), loss_part)
    return (
        loss[0, 0],
        query_grad.reshape(count, 1, query_len, dim),
        passage_grad.reshape(block, 1, tokens, dim),
    )


def solution(mesh):
    return jax.shard_map(
        on_device,
        mesh=mesh,
        in_specs=(
            P("grp", "rep", None, None),
            P("grp", "rep", None, None),
            P("grp", "rep"),
            P("grp", "rep", None),
            P("rep", None),
            P("grp", "rep", None),
            P("grp", "rep"),
        ),
        out_specs=(P(), P("grp", "rep", None, None), P("grp", "rep", None, None)),
        check_vma=False,
    )
```

```python
import functools
import math

import jax
import jax.numpy as jnp
from jax import lax
from jax.experimental import pallas as pl
from jax.experimental.pallas import tpu as pltpu
from jax.sharding import PartitionSpec as P

temper = 0.05
to_base2 = 1.0 / (temper * math.log(2.0))
LANES = 128
MESH = pl.DeviceIdType.MESH
HIGH = lax.Precision.HIGHEST
VMEM_SPEC = pl.BlockSpec(memory_space=pltpu.VMEM)


def greet(groups, replicas, me, mine):
    barrier = pltpu.get_barrier_semaphore()
    for step in range(1, groups):
        pl.semaphore_signal(
            barrier, inc=1, device_id={"grp": lax.rem(me + step, groups)}, device_id_type=MESH
        )
    for step in range(1, replicas):
        pl.semaphore_signal(
            barrier, inc=1, device_id={"rep": lax.rem(mine + step, replicas)}, device_id_type=MESH
        )
    pl.semaphore_wait(barrier, groups - 1 + replicas - 1)


def share_kernel(
    groups, block, queries_ref, cand_ref, map_ref, teacher_ref, weights_ref,
    all_queries, all_meta, query_buf, meta_buf, send_sem, recv_sem,
):
    me = lax.axis_index("grp")
    count, ways = cand_ref.shape
    table = map_ref[...].astype(jnp.float32)
    ids = lax.broadcasted_iota(jnp.int32, (ways, table.shape[1]), 1)
    diagonal = lax.broadcasted_iota(jnp.int32, (ways, ways), 0) == lax.broadcasted_iota(
        jnp.int32, (ways, ways), 1
    )
    teacher = teacher_ref[...]
    top = jnp.max(teacher, axis=1, keepdims=True)
    log_teacher = teacher - top
    log_teacher = log_teacher - jnp.log(jnp.sum(jnp.exp(log_teacher), axis=1, keepdims=True))
    prob = jnp.exp(log_teacher)
    entropy = jnp.sum(prob * log_teacher, axis=1, keepdims=True)
    meta_buf[me] = jnp.zeros(meta_buf.shape[1:], jnp.float32)
    for q in range(count):
        line = cand_ref[q : q + 1, :].astype(jnp.float32)
        column = jnp.sum(jnp.where(diagonal, line, 0.0), axis=1, keepdims=True).astype(jnp.int32)
        row = jnp.sum(jnp.where(column == ids, table, 0.0), axis=1, keepdims=True)
        row = jnp.sum(jnp.where(diagonal, row, 0.0), axis=0, keepdims=True)
        meta_buf[me, q : q + 1, :ways] = row
    meta_buf[me, count : 2 * count, :ways] = prob
    meta_buf[me, 2 * count : 3 * count, :] = jnp.broadcast_to(weights_ref[...], (count, LANES))
    meta_buf[me, 3 * count : 4 * count, :] = jnp.broadcast_to(entropy, (count, LANES))
    query_buf[me] = queries_ref[...]
    greet(groups, 1, me, 0)
    copies = []
    for step in range(1, groups):
        peer = lax.rem(me + step, groups)
        for which, buf in enumerate((query_buf, meta_buf)):
            copies.append(
                pltpu.make_async_remote_copy(
                    src_ref=buf.at[me],
                    dst_ref=buf.at[me],
                    send_sem=send_sem.at[which, step],
                    recv_sem=recv_sem.at[which, step],
                    device_id={"grp": peer},
                    device_id_type=MESH,
                )
            )
            copies[-1].start()
    for copy in copies:
        copy.wait()
    all_queries[...] = query_buf[...]
    all_meta[...] = meta_buf[...]


def span_of(tokens, limit):
    return max(size for size in range(1, limit + 1) if tokens % size == 0)


def lengths_of(lengths_ref, first, rows, width):
    index = lax.broadcasted_iota(jnp.int32, (rows, width), 0)
    found = jnp.zeros((rows, width), jnp.int32)
    for k in range(rows):
        found = jnp.where(index == k, lengths_ref[first + k], found)
    return found


def forward_kernel(
    count, ways, block, lengths_ref, passages_ref, queries_ref, meta_ref,
    lse_ref, score_ref, hits_ref, mass_ref, held, all_lse,
):
    step = pl.program_id(0)
    part = pl.program_id(1)
    groups = meta_ref.shape[0]
    tokens, rows, dim = passages_ref.shape
    width = queries_ref.shape[0]
    slot = score_ref.shape[1]

    @pl.when((step == 0) & (part == 0))
    def _():
        spots = lax.broadcasted_iota(jnp.int32, (ways, groups * slot), 1)
        for source in range(groups):
            turned = jnp.transpose(meta_ref[source])
            for q in range(count):
                row = turned[:ways, q : q + 1].astype(jnp.int32)
                spot = row + (slot - block) * (row // block)
                hot = spot == spots
                place = source * count + q
                hits_ref[place : place + 1, :] = jnp.sum(
                    jnp.where(hot, 1.0, 0.0), axis=0, keepdims=True
                )
                mass_ref[place : place + 1, :] = jnp.sum(
                    jnp.where(hot, turned[:ways, count + q : count + q + 1], 0.0),
                    axis=0,
                    keepdims=True,
                )

    lengths = lengths_of(lengths_ref, step * rows, rows, width)
    size = span_of(tokens, 20)
    highest = jnp.full((rows, width), -1e30, jnp.float32)
    for first in range(0, tokens, size):
        products = lax.dot_general(
            passages_ref[first : first + size].reshape(size * rows, dim), queries_ref[...],
            (((1,), (1,)), ((), ())), preferred_element_type=jnp.float32,
        )
        for j in range(size):
            scaled = jnp.where(
                first + j < lengths, products[j * rows : (j + 1) * rows] * to_base2, -1e30
            )
            held[first + j] = scaled
            highest = jnp.maximum(highest, scaled)
    summed = jnp.zeros((rows, width), jnp.float32)
    for j in range(tokens):
        summed = summed + jnp.exp2(held[j] - highest)
    lse = highest + jnp.log2(summed)
    lse_ref[...] = lse
    all_lse[step, part] = lse

    @pl.when((step == pl.num_programs(0) - 1) & (part == pl.num_programs(1) - 1))
    def _():
        total = score_ref.shape[0]
        parts = all_lse.shape[1]
        each = width * parts // total
        score_ref[...] = jnp.zeros_like(score_ref)
        belongs = lax.broadcasted_iota(jnp.int32, (total // parts, width), 1) // each
        pick = jnp.where(
            belongs == lax.broadcasted_iota(jnp.int32, (total // parts, width), 0), 1.0, 0.0
        )
        span = total // parts
        for k in range(parts):
            matched = jnp.concatenate(
                [all_lse[i, k] for i in range(all_lse.shape[0])], axis=0
            ) * (1.0 / to_base2)
            score_ref[k * span : (k + 1) * span, :block] = lax.dot_general(
                pick, matched, (((1,), (1,)), ((), ())),
                precision=HIGH, preferred_element_type=jnp.float32,
            )


def grade_kernel(
    groups, replicas, score_ref, hits_ref, mass_ref, meta_ref, grad_ref, loss_ref,
    score_buf, weight_buf, grad_buf, query_weight, query_entropy,
    send_sem, recv_sem, wsend_sem, wrecv_sem,
):
    me = lax.axis_index("grp")
    mine = lax.axis_index("rep")
    total, slot = score_ref.shape
    count = total // groups
    for source in range(groups):
        span = slice(source * count, (source + 1) * count)
        query_weight[span, :] = meta_ref[source, 2 * count : 3 * count, :]
        query_entropy[span, :] = meta_ref[source, 3 * count : 4 * count, :]
    weights = query_weight[:, :1]
    score_buf[me] = score_ref[...]
    weight_buf[mine] = jnp.broadcast_to(
        jnp.sum(query_weight[...], axis=0, keepdims=True), weight_buf.shape[1:]
    )
    greet(groups, replicas, me, mine)
    copies = []
    for step in range(1, groups):
        copies.append(
            pltpu.make_async_remote_copy(
                src_ref=score_buf.at[me],
                dst_ref=score_buf.at[me],
                send_sem=send_sem.at[step],
                recv_sem=recv_sem.at[step],
                device_id={"grp": lax.rem(me + step, groups)},
                device_id_type=MESH,
            )
        )
        copies[-1].start()
    for step in range(1, replicas):
        copies.append(
            pltpu.make_async_remote_copy(
                src_ref=weight_buf.at[mine],
                dst_ref=weight_buf.at[mine],
                send_sem=wsend_sem.at[step],
                recv_sem=wrecv_sem.at[step],
                device_id={"rep": lax.rem(mine + step, replicas)},
                device_id_type=MESH,
            )
        )
        copies[-1].start()
    for copy in copies:
        copy.wait()
    weight_sum = jnp.sum(weight_buf[...], axis=0)[:1, :1]
    scores = jnp.concatenate([score_buf[owner] for owner in range(groups)], axis=1)
    hits = hits_ref[...]
    mass = mass_ref[...]
    asked = hits > 0.0
    held = jnp.where(asked, scores, -1e30)
    highest = jnp.max(held, axis=1, keepdims=True)
    summed = jnp.sum(hits * jnp.exp(held - highest), axis=1, keepdims=True)
    log_student = jnp.where(asked, scores - (highest + jnp.log(summed)), -1e30)
    student = hits * jnp.exp(log_student)
    crossed = jnp.sum(jnp.where(asked, mass * log_student, 0.0), axis=1, keepdims=True)
    divergence = query_entropy[:, :1] - crossed
    grad_buf[...] = (total * replicas) * weights / weight_sum * (student - mass)
    own = grad_buf[:, pl.ds(pl.multiple_of(me * slot, slot), slot)]
    width = grad_ref.shape[1]
    each = width // total
    belongs = lax.broadcasted_iota(jnp.int32, (total, width), 1) // each
    pick = jnp.where(belongs == lax.broadcasted_iota(jnp.int32, (total, width), 0), 1.0, 0.0)
    spread = lax.dot_general(
        own, pick, (((0,), (0,)), ((), ())), precision=HIGH, preferred_element_type=jnp.float32
    )
    grad_ref[...] = spread[: grad_ref.shape[0]]
    loss_ref[...] = jnp.broadcast_to(
        jnp.sum(weights * divergence, axis=0, keepdims=True) / weight_sum, loss_ref.shape
    )


def backward_kernel(
    lengths_ref, passages_ref, queries_ref, lse_ref, grad_ref, out_ref, partial_ref,
    total, token_total,
):
    step = pl.program_id(0)
    part = pl.program_id(1)
    parts = total.shape[0]
    tokens, rows, dim = passages_ref.shape
    width = queries_ref.shape[0]

    @pl.when(step == 0)
    def _():
        total[part] = jnp.zeros(total.shape[1:], jnp.float32)

    if parts > 1:

        @pl.when(part == 0)
        def _():
            token_total[...] = jnp.zeros_like(token_total)

    lengths = lengths_of(lengths_ref, step * rows, rows, width)[None]
    lse = lse_ref[...][None]
    grad = grad_ref[...][None]
    queries = queries_ref[...]
    size = span_of(tokens, 36)
    added = None
    for first in range(0, tokens, size):
        passage = passages_ref[first : first + size].reshape(size * rows, dim)
        products = lax.dot_general(
            passage, queries, (((1,), (1,)), ((), ())), preferred_element_type=jnp.float32
        ).reshape(size, rows, width)
        position = first + lax.broadcasted_iota(jnp.int32, (size, 1, 1), 0)
        powers = jnp.exp2(jnp.where(position < lengths, products * to_base2 - lse, -1e30))
        scaled_grad = (powers * grad).astype(jnp.bfloat16).reshape(size * rows, width)
        token_grad = jnp.dot(scaled_grad, queries, preferred_element_type=jnp.float32).reshape(
            size, rows, dim
        )
        if parts > 1:
            token_total[first : first + size] += token_grad
        else:
            out_ref[first : first + size] = token_grad.astype(jnp.bfloat16)
        piece = lax.dot_general(
            passage, scaled_grad, (((0,), (0,)), ((), ())), preferred_element_type=jnp.float32
        )
        added = piece if added is None else added + piece
    total[part] += added

    if parts > 1:

        @pl.when(part == parts - 1)
        def _():
            out_ref[...] = token_total[...].astype(jnp.bfloat16)

    @pl.when(step == pl.num_programs(0) - 1)
    def _():
        partial_ref[pl.ds(pl.multiple_of(part * width, width), width), :] = jnp.transpose(
            total[part]
        ).astype(partial_ref.dtype)


def collect_kernel(
    groups, replicas, partial_ref, loss_ref, grad_ref, loss_out,
    arrived, loss_buf, send_sem, recv_sem, lsend_sem, lrecv_sem,
):
    me = lax.axis_index("grp")
    mine = lax.axis_index("rep")
    loss_buf[mine] = loss_ref[...]
    greet(groups, replicas, me, mine)
    copies = []
    for step in range(1, groups):
        peer = lax.rem(me + step, groups)
        copies.append(
            pltpu.make_async_remote_copy(
                src_ref=partial_ref.at[peer],
                dst_ref=arrived.at[me],
                send_sem=send_sem.at[step],
                recv_sem=recv_sem.at[step],
                device_id={"grp": peer},
                device_id_type=MESH,
            )
        )
        copies[-1].start()
    for step in range(1, replicas):
        copies.append(
            pltpu.make_async_remote_copy(
                src_ref=loss_buf.at[mine],
                dst_ref=loss_buf.at[mine],
                send_sem=lsend_sem.at[step],
                recv_sem=lrecv_sem.at[step],
                device_id={"rep": lax.rem(mine + step, replicas)},
                device_id_type=MESH,
            )
        )
        copies[-1].start()
    arrived[me] = partial_ref[me]
    for copy in copies:
        copy.wait()
    grad_ref[...] = jnp.sum(arrived[...].astype(jnp.float32), axis=0)
    loss_out[...] = jnp.sum(loss_buf[...], axis=0)


def on_device(queries, passages, lengths, cand_ids, owner_map, teacher, weights):
    groups = lax.axis_size("grp")
    replicas = lax.axis_size("rep")
    count, _, query_len, dim = queries.shape
    block, _, tokens, _ = passages.shape
    ways = cand_ids.shape[2]
    own_rows = count * query_len
    width = groups * own_rows
    total = groups * count
    slot = -(-block // LANES) * LANES
    f32 = jnp.float32
    dma = pltpu.SemaphoreType.DMA
    meta_rows = -(-4 * count // 8) * 8
    all_queries, all_meta = pl.pallas_call(
        functools.partial(share_kernel, groups, block),
        name="share",
        out_shape=[
            jax.ShapeDtypeStruct((groups, own_rows, dim), queries.dtype),
            jax.ShapeDtypeStruct((groups, meta_rows, LANES), f32),
        ],
        in_specs=[VMEM_SPEC] * 5,
        out_specs=[VMEM_SPEC] * 2,
        scratch_shapes=[
            pltpu.VMEM((groups, own_rows, dim), queries.dtype),
            pltpu.VMEM((groups, meta_rows, LANES), f32),
            dma((2, groups)),
            dma((2, groups)),
        ],
        compiler_params=pltpu.CompilerParams(collective_id=0, has_side_effects=True),
    )(
        queries.reshape(own_rows, dim),
        cand_ids[:, 0],
        owner_map,
        teacher[:, 0],
        weights,
    )
    flat_queries = all_queries.reshape(width, dim)
    flat_passages = jnp.transpose(passages[:, 0], (1, 0, 2))
    flat_lengths = lengths.reshape(block)
    rows = 16 if block % 16 == 0 else block
    chunk = width if width <= 512 else width // (width // 512)
    parts = width // chunk
    grid = (block // rows, parts)
    whole = lambda *shape: pl.BlockSpec(shape, lambda i, k, *_: (0,) * len(shape))
    passage_spec = pl.BlockSpec((tokens, rows, dim), lambda i, k, *_: (0, i, 0))
    query_spec = pl.BlockSpec((chunk, dim), lambda i, k, *_: (k, 0))
    row_spec = pl.BlockSpec((rows, chunk), lambda i, k, *_: (i, k))
    both = pltpu.CompilerParams(dimension_semantics=("arbitrary", "arbitrary"))
    lse, score, hits, mass = pl.pallas_call(
        functools.partial(forward_kernel, count, ways, block),
        name="forward",
        grid_spec=pltpu.PrefetchScalarGridSpec(
            num_scalar_prefetch=1,
            grid=grid,
            in_specs=[passage_spec, query_spec, whole(groups, meta_rows, LANES)],
            out_specs=[
                row_spec,
                whole(total, slot),
                whole(total, groups * slot),
                whole(total, groups * slot),
            ],
            scratch_shapes=[
                pltpu.VMEM((tokens, rows, chunk), f32),
                pltpu.VMEM((*grid, rows, chunk), f32),
            ],
        ),
        out_shape=[
            jax.ShapeDtypeStruct((block, width), f32),
            jax.ShapeDtypeStruct((total, slot), f32),
            jax.ShapeDtypeStruct((total, groups * slot), f32),
            jax.ShapeDtypeStruct((total, groups * slot), f32),
        ],
        compiler_params=both,
    )(flat_lengths, flat_passages, flat_queries, all_meta)
    grad, loss_part = pl.pallas_call(
        functools.partial(grade_kernel, groups, replicas),
        name="grade",
        out_shape=[
            jax.ShapeDtypeStruct((block, width), f32),
            jax.ShapeDtypeStruct((8, LANES), f32),
        ],
        in_specs=[VMEM_SPEC] * 4,
        out_specs=[VMEM_SPEC] * 2,
        scratch_shapes=[
            pltpu.VMEM((groups, total, slot), f32),
            pltpu.VMEM((replicas, 8, LANES), f32),
            pltpu.VMEM((total, groups * slot), f32),
            pltpu.VMEM((total, LANES), f32),
            pltpu.VMEM((total, LANES), f32),
            dma((groups,)),
            dma((groups,)),
            dma((replicas,)),
            dma((replicas,)),
        ],
        compiler_params=pltpu.CompilerParams(collective_id=1, has_side_effects=True),
    )(score, hits, mass, all_meta)
    passage_grad, partial = pl.pallas_call(
        backward_kernel,
        name="backward",
        grid_spec=pltpu.PrefetchScalarGridSpec(
            num_scalar_prefetch=1,
            grid=grid,
            in_specs=[passage_spec, query_spec, row_spec, row_spec],
            out_specs=[passage_spec, whole(width, dim)],
            scratch_shapes=[
                pltpu.VMEM((parts, dim, chunk), f32),
                pltpu.VMEM((tokens, rows, dim) if parts > 1 else (8, rows, dim), f32),
            ],
        ),
        out_shape=[
            jax.ShapeDtypeStruct((tokens, block, dim), jnp.bfloat16),
            jax.ShapeDtypeStruct((width, dim), jnp.bfloat16),
        ],
        compiler_params=both,
    )(flat_lengths, flat_passages, flat_queries, lse, grad)
    query_grad, loss = pl.pallas_call(
        functools.partial(collect_kernel, groups, replicas),
        name="collect",
        out_shape=[
            jax.ShapeDtypeStruct((own_rows, dim), f32),
            jax.ShapeDtypeStruct((8, LANES), f32),
        ],
        in_specs=[VMEM_SPEC] * 2,
        out_specs=[VMEM_SPEC] * 2,
        scratch_shapes=[
            pltpu.VMEM((groups, own_rows, dim), jnp.bfloat16),
            pltpu.VMEM((replicas, 8, LANES), f32),
            dma((groups,)),
            dma((groups,)),
            dma((replicas,)),
            dma((replicas,)),
        ],
        compiler_params=pltpu.CompilerParams(collective_id=2, has_side_effects=True),
    )(partial.reshape(groups, own_rows, dim), loss_part)
    return (
        loss[0, 0],
        query_grad.reshape(count, 1, query_len, dim),
        jnp.transpose(passage_grad, (1, 0, 2))[:, None],
    )


def solution(mesh):
    return jax.shard_map(
        on_device,
        mesh=mesh,
        in_specs=(
            P("grp", "rep", None, None),
            P("grp", "rep", None, None),
            P("grp", "rep"),
            P("grp", "rep", None),
            P("rep", None),
            P("grp", "rep", None),
            P("grp", "rep"),
        ),
        out_specs=(P(), P("grp", "rep", None, None), P("grp", "rep", None, None)),
        check_vma=False,
    )
```

```python
import functools
import math

import jax
import jax.numpy as jnp
from jax import lax
from jax.experimental import pallas as pl
from jax.experimental.pallas import tpu as pltpu
from jax.sharding import PartitionSpec as P

temper = 0.05
to_base2 = 1.0 / (temper * math.log(2.0))
LANES = 128
MESH = pl.DeviceIdType.MESH
HIGH = lax.Precision.HIGHEST
VMEM_SPEC = pl.BlockSpec(memory_space=pltpu.VMEM)


def greet(groups, replicas, me, mine):
    barrier = pltpu.get_barrier_semaphore()
    for step in range(1, groups):
        pl.semaphore_signal(
            barrier, inc=1, device_id={"grp": lax.rem(me + step, groups)}, device_id_type=MESH
        )
    for step in range(1, replicas):
        pl.semaphore_signal(
            barrier, inc=1, device_id={"rep": lax.rem(mine + step, replicas)}, device_id_type=MESH
        )


def greeted(groups, replicas):
    pl.semaphore_wait(pltpu.get_barrier_semaphore(), groups - 1 + replicas - 1)


def share_kernel(
    groups, block, queries_ref, cand_ref, map_ref, teacher_ref, weights_ref,
    all_queries, all_meta, query_buf, meta_buf, send_sem, recv_sem,
):
    me = lax.axis_index("grp")
    greet(groups, 1, me, 0)
    count, ways = cand_ref.shape
    table = map_ref[...].astype(jnp.float32)
    ids = lax.broadcasted_iota(jnp.int32, (ways, table.shape[1]), 1)
    diagonal = lax.broadcasted_iota(jnp.int32, (ways, ways), 0) == lax.broadcasted_iota(
        jnp.int32, (ways, ways), 1
    )
    teacher = teacher_ref[...]
    top = jnp.max(teacher, axis=1, keepdims=True)
    log_teacher = teacher - top
    log_teacher = log_teacher - jnp.log(jnp.sum(jnp.exp(log_teacher), axis=1, keepdims=True))
    prob = jnp.exp(log_teacher)
    entropy = jnp.sum(prob * log_teacher, axis=1, keepdims=True)
    meta_buf[me] = jnp.zeros(meta_buf.shape[1:], jnp.float32)
    for q in range(count):
        line = cand_ref[q : q + 1, :].astype(jnp.float32)
        column = jnp.sum(jnp.where(diagonal, line, 0.0), axis=1, keepdims=True).astype(jnp.int32)
        row = jnp.sum(jnp.where(column == ids, table, 0.0), axis=1, keepdims=True)
        row = jnp.sum(jnp.where(diagonal, row, 0.0), axis=0, keepdims=True)
        meta_buf[me, q : q + 1, :ways] = row
    meta_buf[me, count : 2 * count, :ways] = prob
    for q in range(count):
        meta_buf[me, 2 * count + q : 2 * count + q + 1, :] = jnp.broadcast_to(
            weights_ref[:, q : q + 1], (1, LANES)
        )
    meta_buf[me, 3 * count : 4 * count, :] = jnp.broadcast_to(entropy, (count, LANES))
    query_buf[me] = queries_ref[...]
    greeted(groups, 1)
    copies = []
    for step in range(1, groups):
        peer = lax.rem(me + step, groups)
        for which, buf in enumerate((query_buf, meta_buf)):
            copies.append(
                pltpu.make_async_remote_copy(
                    src_ref=buf.at[me],
                    dst_ref=buf.at[me],
                    send_sem=send_sem.at[which, step],
                    recv_sem=recv_sem.at[which, step],
                    device_id={"grp": peer},
                    device_id_type=MESH,
                )
            )
            copies[-1].start()
    for copy in copies:
        copy.wait()
    all_queries[...] = query_buf[...]
    all_meta[...] = meta_buf[...]


def span_of(tokens, limit):
    return max(size for size in range(1, limit + 1) if tokens % size == 0)


def lengths_of(lengths_ref, first, rows, width):
    index = lax.broadcasted_iota(jnp.int32, (rows, width), 0)
    found = jnp.zeros((rows, width), jnp.int32)
    for k in range(rows):
        found = jnp.where(index == k, lengths_ref[first + k], found)
    return found


def forward_kernel(
    count, ways, block, lengths_ref, passages_ref, queries_ref, meta_ref,
    lse_ref, score_ref, hits_ref, mass_ref, held, all_lse,
):
    step = pl.program_id(0)
    part = pl.program_id(1)
    groups = meta_ref.shape[0]
    tokens, rows, dim = passages_ref.shape
    width = queries_ref.shape[0]
    slot = score_ref.shape[1]

    @pl.when((step == 0) & (part == 0))
    def _():
        spots = lax.broadcasted_iota(jnp.int32, (ways, groups * slot), 1)
        for source in range(groups):
            turned = jnp.transpose(meta_ref[source])
            for q in range(count):
                row = turned[:ways, q : q + 1].astype(jnp.int32)
                spot = row + (slot - block) * (row // block)
                hot = spot == spots
                place = source * count + q
                hits_ref[place : place + 1, :] = jnp.sum(
                    jnp.where(hot, 1.0, 0.0), axis=0, keepdims=True
                )
                mass_ref[place : place + 1, :] = jnp.sum(
                    jnp.where(hot, turned[:ways, count + q : count + q + 1], 0.0),
                    axis=0,
                    keepdims=True,
                )

    lengths = lengths_of(lengths_ref, step * rows, rows, width)
    size = span_of(tokens, 20)
    highest = jnp.full((rows, width), -1e30, jnp.float32)
    for first in range(0, tokens, size):
        products = lax.dot_general(
            passages_ref[first : first + size].reshape(size * rows, dim), queries_ref[...],
            (((1,), (1,)), ((), ())), preferred_element_type=jnp.float32,
        )
        for j in range(size):
            scaled = jnp.where(
                first + j < lengths, products[j * rows : (j + 1) * rows] * to_base2, -1e30
            )
            held[first + j] = scaled
            highest = jnp.maximum(highest, scaled)
    summed = jnp.zeros((rows, width), jnp.float32)
    for j in range(tokens):
        summed = summed + jnp.exp2(held[j] - highest)
    lse = highest + jnp.log2(summed)
    lse_ref[...] = lse
    all_lse[step, part] = lse

    @pl.when((step == pl.num_programs(0) - 1) & (part == pl.num_programs(1) - 1))
    def _():
        total = score_ref.shape[0]
        parts = all_lse.shape[1]
        each = width * parts // total
        score_ref[...] = jnp.zeros_like(score_ref)
        belongs = lax.broadcasted_iota(jnp.int32, (total // parts, width), 1) // each
        pick = jnp.where(
            belongs == lax.broadcasted_iota(jnp.int32, (total // parts, width), 0), 1.0, 0.0
        )
        span = total // parts
        for k in range(parts):
            matched = jnp.concatenate(
                [all_lse[i, k] for i in range(all_lse.shape[0])], axis=0
            ) * (1.0 / to_base2)
            score_ref[k * span : (k + 1) * span, :block] = lax.dot_general(
                pick, matched, (((1,), (1,)), ((), ())),
                precision=HIGH, preferred_element_type=jnp.float32,
            )


def grade_kernel(
    groups, replicas, score_ref, hits_ref, mass_ref, meta_ref, grad_ref, loss_ref,
    score_buf, weight_buf, grad_buf, query_weight, query_entropy,
    send_sem, recv_sem, wsend_sem, wrecv_sem,
):
    me = lax.axis_index("grp")
    mine = lax.axis_index("rep")
    greet(groups, replicas, me, mine)
    total, slot = score_ref.shape
    count = total // groups
    for source in range(groups):
        span = slice(source * count, (source + 1) * count)
        query_weight[span, :] = meta_ref[source, 2 * count : 3 * count, :]
        query_entropy[span, :] = meta_ref[source, 3 * count : 4 * count, :]
    weights = query_weight[:, :1]
    score_buf[me] = score_ref[...]
    weight_buf[mine] = jnp.broadcast_to(
        jnp.sum(query_weight[...], axis=0, keepdims=True), weight_buf.shape[1:]
    )
    greeted(groups, replicas)
    copies = []
    for step in range(1, groups):
        copies.append(
            pltpu.make_async_remote_copy(
                src_ref=score_buf.at[me],
                dst_ref=score_buf.at[me],
                send_sem=send_sem.at[step],
                recv_sem=recv_sem.at[step],
                device_id={"grp": lax.rem(me + step, groups)},
                device_id_type=MESH,
            )
        )
        copies[-1].start()
    for step in range(1, replicas):
        copies.append(
            pltpu.make_async_remote_copy(
                src_ref=weight_buf.at[mine],
                dst_ref=weight_buf.at[mine],
                send_sem=wsend_sem.at[step],
                recv_sem=wrecv_sem.at[step],
                device_id={"rep": lax.rem(mine + step, replicas)},
                device_id_type=MESH,
            )
        )
        copies[-1].start()
    for copy in copies:
        copy.wait()
    weight_sum = jnp.sum(weight_buf[...], axis=0)[:1, :1]
    scores = jnp.concatenate([score_buf[owner] for owner in range(groups)], axis=1)
    hits = hits_ref[...]
    mass = mass_ref[...]
    asked = hits > 0.0
    held = jnp.where(asked, scores, -1e30)
    highest = jnp.max(held, axis=1, keepdims=True)
    summed = jnp.sum(hits * jnp.exp(held - highest), axis=1, keepdims=True)
    log_student = jnp.where(asked, scores - (highest + jnp.log(summed)), -1e30)
    student = hits * jnp.exp(log_student)
    crossed = jnp.sum(jnp.where(asked, mass * log_student, 0.0), axis=1, keepdims=True)
    divergence = query_entropy[:, :1] - crossed
    grad_buf[...] = (total * replicas) * weights / weight_sum * (student - mass)
    own = grad_buf[:, pl.ds(pl.multiple_of(me * slot, slot), slot)]
    width = grad_ref.shape[1]
    each = width // total
    belongs = lax.broadcasted_iota(jnp.int32, (total, width), 1) // each
    pick = jnp.where(belongs == lax.broadcasted_iota(jnp.int32, (total, width), 0), 1.0, 0.0)
    spread = lax.dot_general(
        own, pick, (((0,), (0,)), ((), ())), precision=HIGH, preferred_element_type=jnp.float32
    )
    grad_ref[...] = spread[: grad_ref.shape[0]]
    loss_ref[...] = jnp.broadcast_to(
        jnp.sum(weights * divergence, axis=0, keepdims=True) / weight_sum, loss_ref.shape
    )


def backward_kernel(
    lengths_ref, passages_ref, queries_ref, lse_ref, grad_ref, out_ref, partial_ref,
    total, token_total,
):
    step = pl.program_id(0)
    part = pl.program_id(1)
    parts = total.shape[0]
    tokens, rows, dim = passages_ref.shape
    width = queries_ref.shape[0]

    @pl.when(step == 0)
    def _():
        total[part] = jnp.zeros(total.shape[1:], jnp.float32)

    if parts > 1:

        @pl.when(part == 0)
        def _():
            token_total[...] = jnp.zeros_like(token_total)

    lengths = lengths_of(lengths_ref, step * rows, rows, width)[None]
    lse = lse_ref[...][None]
    grad = grad_ref[...][None]
    queries = queries_ref[...]
    size = span_of(tokens, 36)
    added = None
    for first in range(0, tokens, size):
        passage = passages_ref[first : first + size].reshape(size * rows, dim)
        products = lax.dot_general(
            passage, queries, (((1,), (1,)), ((), ())), preferred_element_type=jnp.float32
        ).reshape(size, rows, width)
        position = first + lax.broadcasted_iota(jnp.int32, (size, 1, 1), 0)
        powers = jnp.exp2(jnp.where(position < lengths, products * to_base2 - lse, -1e30))
        scaled_grad = (powers * grad).astype(jnp.bfloat16).reshape(size * rows, width)
        token_grad = jnp.dot(scaled_grad, queries, preferred_element_type=jnp.float32).reshape(
            size, rows, dim
        )
        if parts > 1:
            token_total[first : first + size] += token_grad
        else:
            out_ref[first : first + size] = token_grad.astype(jnp.bfloat16)
        piece = lax.dot_general(
            passage, scaled_grad, (((0,), (0,)), ((), ())), preferred_element_type=jnp.float32
        )
        added = piece if added is None else added + piece
    total[part] += added

    if parts > 1:

        @pl.when(part == parts - 1)
        def _():
            out_ref[...] = token_total[...].astype(jnp.bfloat16)

    @pl.when(step == pl.num_programs(0) - 1)
    def _():
        partial_ref[pl.ds(pl.multiple_of(part * width, width), width), :] = jnp.transpose(
            total[part]
        ).astype(partial_ref.dtype)


def collect_kernel(
    groups, replicas, partial_ref, loss_ref, grad_ref, loss_out,
    arrived, loss_buf, send_sem, recv_sem, lsend_sem, lrecv_sem,
):
    me = lax.axis_index("grp")
    mine = lax.axis_index("rep")
    greet(groups, replicas, me, mine)
    loss_buf[mine] = loss_ref[...]
    greeted(groups, replicas)
    copies = []
    for step in range(1, groups):
        peer = lax.rem(me + step, groups)
        copies.append(
            pltpu.make_async_remote_copy(
                src_ref=partial_ref.at[peer],
                dst_ref=arrived.at[me],
                send_sem=send_sem.at[step],
                recv_sem=recv_sem.at[step],
                device_id={"grp": peer},
                device_id_type=MESH,
            )
        )
        copies[-1].start()
    for step in range(1, replicas):
        copies.append(
            pltpu.make_async_remote_copy(
                src_ref=loss_buf.at[mine],
                dst_ref=loss_buf.at[mine],
                send_sem=lsend_sem.at[step],
                recv_sem=lrecv_sem.at[step],
                device_id={"rep": lax.rem(mine + step, replicas)},
                device_id_type=MESH,
            )
        )
        copies[-1].start()
    arrived[me] = partial_ref[me]
    for copy in copies:
        copy.wait()
    grad_ref[...] = jnp.sum(arrived[...].astype(jnp.float32), axis=0)
    loss_out[...] = jnp.sum(loss_buf[...], axis=0)[:1, :1]


def on_device(queries, passages, lengths, cand_ids, owner_map, teacher, weights):
    groups = lax.axis_size("grp")
    replicas = lax.axis_size("rep")
    count, _, query_len, dim = queries.shape
    block, _, tokens, _ = passages.shape
    ways = cand_ids.shape[2]
    own_rows = count * query_len
    width = groups * own_rows
    total = groups * count
    slot = -(-block // LANES) * LANES
    f32 = jnp.float32
    dma = pltpu.SemaphoreType.DMA
    meta_rows = -(-4 * count // 8) * 8
    all_queries, all_meta = pl.pallas_call(
        functools.partial(share_kernel, groups, block),
        name="share",
        out_shape=[
            jax.ShapeDtypeStruct((groups, own_rows, dim), queries.dtype),
            jax.ShapeDtypeStruct((groups, meta_rows, LANES), f32),
        ],
        in_specs=[VMEM_SPEC] * 5,
        out_specs=[VMEM_SPEC] * 2,
        scratch_shapes=[
            pltpu.VMEM((groups, own_rows, dim), queries.dtype),
            pltpu.VMEM((groups, meta_rows, LANES), f32),
            dma((2, groups)),
            dma((2, groups)),
        ],
        compiler_params=pltpu.CompilerParams(collective_id=0, has_side_effects=True),
    )(
        queries.reshape(own_rows, dim),
        cand_ids[:, 0],
        owner_map,
        teacher[:, 0],
        jnp.transpose(weights),
    )
    flat_queries = all_queries.reshape(width, dim)
    flat_passages = jnp.transpose(passages[:, 0], (1, 0, 2))
    flat_lengths = lengths.reshape(block)
    rows = 16 if block % 16 == 0 else block
    chunk = width if width <= 512 else width // (width // 512)
    parts = width // chunk
    grid = (block // rows, parts)
    whole = lambda *shape: pl.BlockSpec(shape, lambda i, k, *_: (0,) * len(shape))
    passage_spec = pl.BlockSpec((tokens, rows, dim), lambda i, k, *_: (0, i, 0))
    query_spec = pl.BlockSpec((chunk, dim), lambda i, k, *_: (k, 0))
    row_spec = pl.BlockSpec((rows, chunk), lambda i, k, *_: (i, k))
    both = pltpu.CompilerParams(dimension_semantics=("arbitrary", "arbitrary"))
    lse, score, hits, mass = pl.pallas_call(
        functools.partial(forward_kernel, count, ways, block),
        name="forward",
        grid_spec=pltpu.PrefetchScalarGridSpec(
            num_scalar_prefetch=1,
            grid=grid,
            in_specs=[passage_spec, query_spec, whole(groups, meta_rows, LANES)],
            out_specs=[
                row_spec,
                whole(total, slot),
                whole(total, groups * slot),
                whole(total, groups * slot),
            ],
            scratch_shapes=[
                pltpu.VMEM((tokens, rows, chunk), f32),
                pltpu.VMEM((*grid, rows, chunk), f32),
            ],
        ),
        out_shape=[
            jax.ShapeDtypeStruct((block, width), f32),
            jax.ShapeDtypeStruct((total, slot), f32),
            jax.ShapeDtypeStruct((total, groups * slot), f32),
            jax.ShapeDtypeStruct((total, groups * slot), f32),
        ],
        compiler_params=both,
    )(flat_lengths, flat_passages, flat_queries, all_meta)
    grad, loss_part = pl.pallas_call(
        functools.partial(grade_kernel, groups, replicas),
        name="grade",
        out_shape=[
            jax.ShapeDtypeStruct((block, width), f32),
            jax.ShapeDtypeStruct((8, LANES), f32),
        ],
        in_specs=[VMEM_SPEC] * 4,
        out_specs=[VMEM_SPEC] * 2,
        scratch_shapes=[
            pltpu.VMEM((groups, total, slot), f32),
            pltpu.VMEM((replicas, 8, LANES), f32),
            pltpu.VMEM((total, groups * slot), f32),
            pltpu.VMEM((total, LANES), f32),
            pltpu.VMEM((total, LANES), f32),
            dma((groups,)),
            dma((groups,)),
            dma((replicas,)),
            dma((replicas,)),
        ],
        compiler_params=pltpu.CompilerParams(collective_id=1, has_side_effects=True),
    )(score, hits, mass, all_meta)
    passage_grad, partial = pl.pallas_call(
        backward_kernel,
        name="backward",
        grid_spec=pltpu.PrefetchScalarGridSpec(
            num_scalar_prefetch=1,
            grid=grid,
            in_specs=[passage_spec, query_spec, row_spec, row_spec],
            out_specs=[passage_spec, whole(width, dim)],
            scratch_shapes=[
                pltpu.VMEM((parts, dim, chunk), f32),
                pltpu.VMEM((tokens, rows, dim) if parts > 1 else (8, rows, dim), f32),
            ],
        ),
        out_shape=[
            jax.ShapeDtypeStruct((tokens, block, dim), jnp.bfloat16),
            jax.ShapeDtypeStruct((width, dim), jnp.bfloat16),
        ],
        compiler_params=both,
    )(flat_lengths, flat_passages, flat_queries, lse, grad)
    query_grad, loss = pl.pallas_call(
        functools.partial(collect_kernel, groups, replicas),
        name="collect",
        out_shape=[
            jax.ShapeDtypeStruct((own_rows, dim), f32),
            jax.ShapeDtypeStruct((1, 1), f32),
        ],
        in_specs=[VMEM_SPEC] * 2,
        out_specs=[VMEM_SPEC] * 2,
        scratch_shapes=[
            pltpu.VMEM((groups, own_rows, dim), jnp.bfloat16),
            pltpu.VMEM((replicas, 8, LANES), f32),
            dma((groups,)),
            dma((groups,)),
            dma((replicas,)),
            dma((replicas,)),
        ],
        compiler_params=pltpu.CompilerParams(collective_id=2, has_side_effects=True),
    )(partial.reshape(groups, own_rows, dim), loss_part)
    return (
        loss.reshape(()),
        query_grad.reshape(count, 1, query_len, dim),
        jnp.transpose(passage_grad, (1, 0, 2))[:, None],
    )


def solution(mesh):
    return jax.shard_map(
        on_device,
        mesh=mesh,
        in_specs=(
            P("grp", "rep", None, None),
            P("grp", "rep", None, None),
            P("grp", "rep"),
            P("grp", "rep", None),
            P("rep", None),
            P("grp", "rep", None),
            P("grp", "rep"),
        ),
        out_specs=(P(), P("grp", "rep", None, None), P("grp", "rep", None, None)),
        check_vma=False,
    )
```
